32 devices in a mesh: dp: 1 (over z), tp: 32 (over y, x, core).
Axes of the slice: x: 4, y: 4, z: 1, core: 2. Of those that a mesh axis runs over, the one named last changes fastest.
The devices are a block of a 4x4x8 slice.
Arguments:
- token_ids: int32 [4096], P('dp')
- emb_table: bfloat16 [51200, 2560], P('tp')
- norm_gain: bfloat16 [2560], replicated
- w_in: bfloat16 [2560, 10240], P(None, 'tp')
- w_out: bfloat16 [10240, 2560], P('tp')
- d_out: bfloat16 [4096, 2560], P(('dp', 'tp'))
Outputs:
- output 1: bfloat16 [4096, 2560], P(('dp', 'tp'))
- output 2: float32 [51200, 2560], P(('dp', 'tp'))
- output 3: float32 [2560, 10240], P('dp', 'tp')
- output 4: float32 [10240, 2560], P(('dp', 'tp'))
All inputs are finite; a program needn't handle non-finite values.
Results may differ from the reference program's by a relative error of at most 0.00843216.
Values are sent between devices in bfloat16 or wider.
A program may use at most 768 MiB of HBM per device.

```python
import math
import jax
import jax.numpy as jnp
from jax import lax

VOCAB_SIZE = 51200
MODEL_DIM = 2560
HIDDEN_DIM = 10240
TOKENS = 4096

EPS = 1e-6
VOCAB_BITS = math.ceil(math.log2(VOCAB_SIZE))


def draw_ids(id_key):
    key_level, key_zipf, key_flat, key_pick = jax.random.split(id_key, 4)
    bit_level = jax.random.randint(key_level, (TOKENS,), 0, VOCAB_BITS + 1, dtype=jnp.int32)
    id_span = jnp.left_shift(jnp.ones_like(bit_level), bit_level)
    zipf_ids = jax.random.randint(key_zipf, (TOKENS,), 0, id_span, dtype=jnp.int32) % VOCAB_SIZE
    flat_ids = jax.random.randint(key_flat, (TOKENS,), 0, VOCAB_SIZE, dtype=jnp.int32)
    choice = jax.random.randint(key_pick, (TOKENS,), 0, 10, dtype=jnp.int32)
    mixed_ids = jnp.where(choice < 7, zipf_ids, flat_ids)
    end_ids = jnp.array([0, VOCAB_SIZE - 1], dtype=jnp.int32)
    return jnp.concatenate([end_ids, mixed_ids[2:]]).astype(jnp.int32)


def setup_inputs(seed: int = 0, part: int = 0) -> dict:
    key_table, key_gain, key_in, key_out = jax.random.split(jax.random.key(seed), 4)
    part_key = jax.random.fold_in(jax.random.key(seed + 1), part)
    key_ids, key_dout = jax.random.split(part_key, 2)
    emb_table = jax.random.normal(key_table, (VOCAB_SIZE, MODEL_DIM), jnp.float32).astype(jnp.bfloat16)
    norm_gain = (1.0 + 0.5 * jax.random.normal(key_gain, (MODEL_DIM,), jnp.float32)).astype(jnp.bfloat16)
    w_in = (jax.random.normal(key_in, (MODEL_DIM, HIDDEN_DIM), jnp.float32) * MODEL_DIM ** -0.5).astype(jnp.bfloat16)
    w_out = (jax.random.normal(key_out, (HIDDEN_DIM, MODEL_DIM), jnp.float32) * (1.5 * HIDDEN_DIM ** -0.5)).astype(jnp.bfloat16)
    token_ids = draw_ids(key_ids)
    d_out = (jax.random.normal(key_dout, (TOKENS, MODEL_DIM), jnp.float32) * TOKENS ** -0.5).astype(jnp.bfloat16)
    return {"token_ids": token_ids, "emb_table": emb_table, "norm_gain": norm_gain, "w_in": w_in, "w_out": w_out, "d_out": d_out}


def reference(token_ids, emb_table, norm_gain, w_in, w_out, d_out):
    embedded = jnp.take(emb_table, token_ids, axis=0)
    embedded_f32 = embedded.astype(jnp.float32)
    inv_rms = lax.rsqrt(jnp.mean(embedded_f32 * embedded_f32, axis=-1, keepdims=True) + EPS)
    gain_f32 = norm_gain.astype(jnp.float32)
    normed = (embedded_f32 * inv_rms * gain_f32).astype(jnp.bfloat16)
    pre_act = jnp.dot(normed, w_in, preferred_element_type=jnp.float32).astype(jnp.bfloat16)
    act_f32, gelu_vjp = jax.vjp(jax.nn.gelu, pre_act.astype(jnp.float32))
    hidden = act_f32.astype(jnp.bfloat16)
    mlp_out = jnp.dot(hidden, w_out, preferred_element_type=jnp.float32)
    block_out = (embedded_f32 + mlp_out).astype(jnp.bfloat16)
    d_hidden = jnp.dot(d_out, w_out.T, preferred_element_type=jnp.float32).astype(jnp.bfloat16)
    d_w_out = jnp.dot(hidden.T, d_out, preferred_element_type=jnp.float32)
    (d_pre_f32,) = gelu_vjp(d_hidden.astype(jnp.float32))
    d_pre = d_pre_f32.astype(jnp.bfloat16)
    d_w_in = jnp.dot(normed.T, d_pre, preferred_element_type=jnp.float32)
    d_normed = jnp.dot(d_pre, w_in.T, preferred_element_type=jnp.float32)
    d_scaled = d_normed * gain_f32
    row_proj = jnp.mean(d_scaled * embedded_f32, axis=-1, keepdims=True)
    d_emb = (d_out.astype(jnp.float32) + inv_rms * (d_scaled - embedded_f32 * inv_rms * inv_rms * row_proj)).astype(jnp.bfloat16)
    d_table = jax.ops.segment_sum(d_emb.astype(jnp.float32), token_ids, num_segments=VOCAB_SIZE)
    return block_out, d_table, d_w_in, d_w_out
```

```python
import jax
import jax.numpy as jnp
from jax import lax
from jax.sharding import PartitionSpec as P

EPS = 1e-6
CHUNKS = 2


def solution(mesh):
    n_dev = mesh.shape["tp"]
    planes = [list(range(c, n_dev, 2)) for c in range(2)]
    swap = [(i, i ^ 1) for i in range(n_dev)]
    f32, bf16 = jnp.float32, jnp.bfloat16

    def gather_plane(v):
        return lax.all_gather(v, "tp", axis=0, tiled=True, axis_index_groups=planes)

    def scatter_plane(v):
        return lax.psum_scatter(v, "tp", scatter_dimension=0, tiled=True, axis_index_groups=planes)

    def dot(a, b, ca, cb):
        return lax.dot_general(a, b, (((ca,), (cb,)), ((), ())), preferred_element_type=f32)

    def shard_step(token_ids, emb_table, norm_gain, w_in, w_out, d_out):
        rank = lax.axis_index("tp")
        core = rank % 2
        rows = d_out.shape[0]
        width = w_in.shape[1]
        vocab = emb_table.shape[0]
        part = rows // CHUNKS
        own_base = rank * vocab
        sib_base = (rank + 1 - 2 * core) * vocab
        ids_blocks = token_ids.reshape(n_dev // 2, 2, rows)
        ids_plane = lax.dynamic_index_in_dim(ids_blocks, core, axis=1, keepdims=False).reshape(-1, 1)
        vocab_col = lax.broadcasted_iota(jnp.int32, (1, vocab), 1)
        vocab_row = lax.broadcasted_iota(jnp.int32, (vocab, 1), 0)
        gain_f32 = norm_gain.astype(f32)

        table_sib = lax.ppermute(emb_table, "tp", swap)
        w_out2 = jnp.concatenate([w_out, lax.ppermute(w_out, "tp", swap)], axis=0)
        w_in2 = jnp.concatenate([w_in, lax.ppermute(w_in, "tp", swap)], axis=1)

        d_full = gather_plane(d_out)

        own = (ids_plane - own_base == vocab_col).astype(bf16)
        sib = (ids_plane - sib_base == vocab_col).astype(bf16)
        look = (dot(own, emb_table, 1, 0) + dot(sib, table_sib, 1, 0)).astype(bf16)
        look, d_full = lax.optimization_barrier((look, d_full))
        emb = scatter_plane(look).astype(f32)
        inv = lax.rsqrt(jnp.mean(emb * emb, axis=-1, keepdims=True) + EPS)
        normed_local = (emb * inv * gain_f32).astype(bf16)
        normed = [gather_plane(normed_local[k * part:(k + 1) * part]) for k in range(CHUNKS)]

        d_hidden = dot(d_full, w_out2, 1, 1).astype(bf16)
        d_hidden_c = d_hidden.reshape(n_dev // 2, CHUNKS, part, 2 * width)
        hidden, d_pre, d_normed = [], [], []
        for k in range(CHUNKS):
            pre_act = dot(normed[k], w_in2, 1, 0).astype(bf16)
            act_f32, gelu_vjp = jax.vjp(jax.nn.gelu, pre_act.astype(f32))
            hidden.append(act_f32.astype(bf16).reshape(n_dev // 2, 1, part, 2 * width))
            (d_pre_f32,) = gelu_vjp(d_hidden_c[:, k].reshape(-1, 2 * width).astype(f32))
            d_pre.append(d_pre_f32.astype(bf16))
            d_normed.append(scatter_plane(dot(d_pre[k], w_in2, 1, 1)))
        hidden = jnp.concatenate(hidden, axis=1).reshape(-1, 2 * width)
        y_part = dot(hidden, w_out2, 1, 0)

        d_w_in2 = sum(dot(normed[k], d_pre[k], 0, 0) for k in range(CHUNKS))
        d_w_out2 = dot(hidden, d_full, 0, 0)
        d_w_in = d_w_in2[:, :width] + lax.ppermute(d_w_in2[:, width:], "tp", swap)
        d_w_out = d_w_out2[:width] + lax.ppermute(d_w_out2[width:], "tp", swap)

        d_scaled = jnp.concatenate(d_normed, axis=0) * gain_f32
        row_proj = jnp.mean(d_scaled * emb, axis=-1, keepdims=True)
        d_emb = (d_out.astype(f32) + inv * (d_scaled - emb * inv * inv * row_proj)).astype(bf16)
        d_emb_full = lax.all_gather(d_emb, "tp", axis=0, tiled=True)
        y_part, d_emb_full = lax.optimization_barrier((y_part, d_emb_full))
        block_out = (emb + scatter_plane(y_part)).astype(bf16)

        hit = (token_ids.reshape(1, -1) - own_base == vocab_row).astype(bf16)
        d_table = dot(hit, d_emb_full, 1, 0)
        return block_out, d_table, d_w_in, d_w_out

    return jax.shard_map(
        shard_step,
        mesh=mesh,
        in_specs=(P("dp"), P("tp", None), P(None), P(None, "tp"), P("tp", None), P(("dp", "tp"), None)),
        out_specs=(P(("dp", "tp"), None), P(("dp", "tp"), None), P("dp", "tp"), P(("dp", "tp"), None)),
        check_vma=False,
    )
```

```python
import functools
import math

import jax
import jax.numpy as jnp
from jax import lax
from jax.experimental import pallas as pl
from jax.experimental.pallas import tpu as pltpu
from jax.sharding import PartitionSpec as P

EPS = 1e-6
STREAMS = 4


def exchange_kernel(side, gain_ref, look_ref, x_ref, n_ref, ring1, ring2, s1, r1, s2, r2, t1, u1, t2, u2):
    rows, dim = x_ref.shape
    cols = dim // STREAMS
    rank = lax.axis_index("tp")
    core = lax.rem(rank, 2)
    chip = rank // 2
    y, x = chip // side, lax.rem(chip, side)
    last = side - 1

    def wrap(v):
        return lax.rem(v + 2 * side, side)

    def device(yy, xx):
        return {"tp": (wrap(yy) * side + wrap(xx)) * 2 + core}

    def sign(k):
        return 1 if k % 2 == 0 else -1

    def first(k):
        return x if k < 2 else y

    def second(k):
        return y if k < 2 else x

    def piece(ref, k, a, b):
        block = (wrap(b) * side + wrap(a)) if k < 2 else (wrap(a) * side + wrap(b))
        return ref.at[pl.ds(pl.multiple_of(block * rows, rows), rows), pl.ds(k * cols, cols)]

    def next_first(k):
        return device(y, x + sign(k)) if k < 2 else device(y + sign(k), x)

    def next_second(k):
        return device(y + sign(k), x) if k < 2 else device(y, x + sign(k))

    def copy(src, dst, send, recv, to):
        return pltpu.make_async_remote_copy(
            src_ref=src, dst_ref=dst, send_sem=send, recv_sem=recv, device_id=to, device_id_type=pl.DeviceIdType.MESH
        )

    barrier = pltpu.get_barrier_semaphore()
    for dy, dx in ((0, 1), (0, -1), (1, 0), (-1, 0)):
        pl.semaphore_signal(barrier, inc=1, device_id=device(y + dy, x + dx), device_id_type=pl.DeviceIdType.MESH)
    pl.semaphore_wait(barrier, 4)

    every = range(STREAMS)
    sent = []

    def scatter_first(k, s, j, src):
        return copy(src, ring1.at[k, s, j], s1.at[k, s, j], r1.at[k, s, j], next_first(k))

    def scatter_second(k, m, src):
        return copy(src, ring2.at[k, m], s2.at[k, m], r2.at[k, m], next_second(k))

    def go(c):
        c.start()
        sent.append(c)

    for j in range(side):
        for k in every:
            go(scatter_first(k, 0, j, piece(look_ref, k, first(k) - sign(k), second(k) - sign(k) * (1 + j))))
    for s in range(last):
        for j in range(side):
            for k in every:
                held = ring1.at[k, s, j]
                scatter_first(k, s, j, held).wait_recv()
                own = piece(look_ref, k, first(k) - sign(k) * (2 + s), second(k) - sign(k) * (1 + j))
                held[...] += own[...]
            for k in every:
                held = ring1.at[k, s, j]
                if s < last - 1:
                    go(scatter_first(k, s + 1, j, held))
                elif j == 0:
                    go(scatter_second(k, 0, held))
    for j in range(1, side):
        for k in every:
            held = ring2.at[k, j - 1]
            scatter_second(k, j - 1, held).wait_recv()
            total = held[...] + ring1[k, last - 1, j]
            if j < last:
                held[...] = total
            else:
                x_ref[:, pl.ds(k * cols, cols)] = total
        if j < last:
            for k in every:
                go(scatter_second(k, j, ring2.at[k, j - 1]))

    mine = pl.multiple_of(chip * rows, rows)
    strip = 16

    @pl.loop(0, rows // strip)
    def _(i):
        at = pl.ds(pl.multiple_of(i * strip, strip), strip)
        e = x_ref[at, :].astype(jnp.float32)
        r = lax.rsqrt(jnp.mean(e * e, axis=-1, keepdims=True) + EPS)
        n_ref[pl.ds(pl.multiple_of(mine + i * strip, strip), strip), :] = (
            e * r * gain_ref[...].astype(jnp.float32)
        ).astype(jnp.bfloat16)

    def gather_first(k, s):
        p = piece(n_ref, k, first(k) - sign(k) * s, second(k))
        return copy(p, p, t1.at[k, s], u1.at[k, s], next_first(k))

    def gather_second(k, m, i):
        p = piece(n_ref, k, first(k) - sign(k) * i, second(k) - sign(k) * m)
        return copy(p, p, t2.at[k, m, i], u2.at[k, m, i], next_second(k))

    def arrived_first(k, s):
        p = piece(n_ref, k, first(k) - sign(k) * (s + 1), second(k))
        copy(p, p, t1.at[k, s], u1.at[k, s], next_first(k)).wait_recv()

    def arrived_second(k, m, i):
        p = piece(n_ref, k, first(k) - sign(k) * i, second(k) - sign(k) * (m + 1))
        copy(p, p, t2.at[k, m, i], u2.at[k, m, i], next_second(k)).wait_recv()
        if m < last - 1:
            go(gather_second(k, m + 1, i))

    for k in every:
        go(gather_first(k, 0))
        go(gather_second(k, 0, 0))
    for s in range(last):
        for k in every:
            arrived_first(k, s)
            if s < last - 1:
                go(gather_first(k, s + 1))
            go(gather_second(k, 0, s + 1))
        for k in every:
            arrived_second(k, 0, s)
    for m in range(last):
        for i in range(last if m == 0 else 0, side):
            for k in every:
                arrived_second(k, m, i)
    for c in sent:
        c.wait_send()


def exchange(look, gain, rows, side):
    total, dim = look.shape
    cols = dim // STREAMS
    last = side - 1
    dma = pltpu.SemaphoreType.DMA
    vmem = pl.BlockSpec(memory_space=pltpu.VMEM)
    return pl.pallas_call(
        functools.partial(exchange_kernel, side),
        out_shape=(jax.ShapeDtypeStruct((rows, dim), look.dtype), jax.ShapeDtypeStruct((total, dim), look.dtype)),
        in_specs=[vmem, vmem],
        out_specs=(vmem, vmem),
        scratch_shapes=[
            pltpu.VMEM((STREAMS, last, side, rows, cols), look.dtype),
            pltpu.VMEM((STREAMS, last, rows, cols), look.dtype),
            dma((STREAMS, last, side)),
            dma((STREAMS, last, side)),
            dma((STREAMS, last)),
            dma((STREAMS, last)),
            dma((STREAMS, last)),
            dma((STREAMS, last)),
            dma((STREAMS, last, side)),
            dma((STREAMS, last, side)),
        ],
        compiler_params=pltpu.CompilerParams(collective_id=0, has_side_effects=True),
        cost_estimate=pl.CostEstimate(flops=100_000_000_000, bytes_accessed=4 * total * dim, transcendentals=0),
        name="exchange",
    )(gain.reshape(1, dim), look)


def solution(mesh):
    n_dev = mesh.shape["tp"]
    planes = [list(range(c, n_dev, 2)) for c in range(2)]
    side = math.isqrt(n_dev // 2)
    swap = [(i, i ^ 1) for i in range(n_dev)]
    f32, bf16 = jnp.float32, jnp.bfloat16

    def gather_plane(v):
        return lax.all_gather(v, "tp", axis=0, tiled=True, axis_index_groups=planes)

    def scatter_plane(v):
        return lax.psum_scatter(v, "tp", scatter_dimension=0, tiled=True, axis_index_groups=planes)

    def dot(a, b, ca, cb):
        return lax.dot_general(a, b, (((ca,), (cb,)), ((), ())), preferred_element_type=f32)

    def shard_step(token_ids, emb_table, norm_gain, w_in, w_out, d_out):
        rank = lax.axis_index("tp")
        core = rank % 2
        rows = d_out.shape[0]
        width = w_in.shape[1]
        vocab = emb_table.shape[0]
        own_base = rank * vocab
        sib_base = (rank + 1 - 2 * core) * vocab
        ids_blocks = token_ids.reshape(n_dev // 2, 2, rows)
        ids_plane = lax.dynamic_index_in_dim(ids_blocks, core, axis=1, keepdims=False).reshape(-1, 1)
        vocab_col = lax.broadcasted_iota(jnp.int32, (1, vocab), 1)
        vocab_row = lax.broadcasted_iota(jnp.int32, (vocab, 1), 0)
        gain_f32 = norm_gain.astype(f32)

        table_sib = lax.ppermute(emb_table, "tp", swap)
        w_out2 = jnp.concatenate([w_out, lax.ppermute(w_out, "tp", swap)], axis=0)
        w_in2 = jnp.concatenate([w_in, lax.ppermute(w_in, "tp", swap)], axis=1)

        d_full = gather_plane(d_out)

        own = (ids_plane - own_base == vocab_col).astype(bf16)
        sib = (ids_plane - sib_base == vocab_col).astype(bf16)
        look = (dot(own, emb_table, 1, 0) + dot(sib, table_sib, 1, 0)).astype(bf16)
        emb, normed = exchange(look, norm_gain, rows, side)
        emb = emb.astype(f32)
        inv = lax.rsqrt(jnp.mean(emb * emb, axis=-1, keepdims=True) + EPS)

        d_hidden = dot(d_full, w_out2, 1, 1).astype(bf16)
        pre_act = dot(normed, w_in2, 1, 0).astype(bf16)
        act_f32, gelu_vjp = jax.vjp(jax.nn.gelu, pre_act.astype(f32))
        hidden = act_f32.astype(bf16)
        (d_pre_f32,) = gelu_vjp(d_hidden.astype(f32))
        d_pre = d_pre_f32.astype(bf16)
        d_normed = scatter_plane(dot(d_pre, w_in2, 1, 1))
        y_part = dot(hidden, w_out2, 1, 0)

        d_w_in2 = dot(normed, d_pre, 0, 0)
        d_w_out2 = dot(hidden, d_full, 0, 0)
        d_w_in = d_w_in2[:, :width] + lax.ppermute(d_w_in2[:, width:], "tp", swap)
        d_w_out = d_w_out2[:width] + lax.ppermute(d_w_out2[width:], "tp", swap)

        d_scaled = d_normed * gain_f32
        row_proj = jnp.mean(d_scaled * emb, axis=-1, keepdims=True)
        d_emb = (d_out.astype(f32) + inv * (d_scaled - emb * inv * inv * row_proj)).astype(bf16)
        d_emb_full = lax.all_gather(d_emb, "tp", axis=0, tiled=True)
        y_part, d_emb_full = lax.optimization_barrier((y_part, d_emb_full))
        block_out = (emb + scatter_plane(y_part)).astype(bf16)

        hit = (token_ids.reshape(1, -1) - own_base == vocab_row).astype(bf16)
        d_table = dot(hit, d_emb_full, 1, 0)
        return block_out, d_table, d_w_in, d_w_out

    return jax.shard_map(
        shard_step,
        mesh=mesh,
        in_specs=(P("dp"), P("tp", None), P(None), P(None, "tp"), P("tp", None), P(("dp", "tp"), None)),
        out_specs=(P(("dp", "tp"), None), P(("dp", "tp"), None), P("dp", "tp"), P(("dp", "tp"), None)),
        check_vma=False,
    )
```

```python
import functools
import math

import jax
import jax.numpy as jnp
from jax import lax
from jax.experimental import pallas as pl
from jax.experimental.pallas import tpu as pltpu
from jax.sharding import PartitionSpec as P

EPS = 1e-6
STREAMS = 4


MESH = pl.DeviceIdType.MESH


class Plane:
    def __init__(self, side, rows, cols, cores=1):
        self.side, self.rows, self.cols, self.cores = side, rows, cols, cores
        self.rank = lax.axis_index("tp")
        self.core = lax.rem(self.rank, 2)
        self.chip = self.rank // 2
        self.y, self.x = self.chip // side, lax.rem(self.chip, side)

    def wrap(self, v):
        return lax.rem(v + 2 * self.side, self.side)

    def device(self, yy, xx):
        return {"tp": (self.wrap(yy) * self.side + self.wrap(xx)) * 2 + self.core}

    def sibling(self):
        return {"tp": self.chip * 2 + 1 - self.core}

    def sign(self, k):
        return 1 if k % 2 == 0 else -1

    def first(self, k):
        return self.x if k < 2 else self.y

    def second(self, k):
        return self.y if k < 2 else self.x

    def block_rows(self, k, a, b, core=0):
        a = self.wrap(self.first(k) - self.sign(k) * a)
        b = self.wrap(self.second(k) - self.sign(k) * b)
        block = ((b * self.side + a) if k < 2 else (a * self.side + b)) * self.cores + core
        start = pl.multiple_of(block * self.rows, self.rows)
        return pl.ds(start, self.rows)

    def piece(self, ref, k, a, b, core=0):
        return ref.at[self.block_rows(k, a, b, core), pl.ds(k * self.cols, self.cols)]

    def next_first(self, k):
        return self.device(self.y, self.x + self.sign(k)) if k < 2 else self.device(self.y + self.sign(k), self.x)

    def next_second(self, k):
        return self.device(self.y + self.sign(k), self.x) if k < 2 else self.device(self.y, self.x + self.sign(k))

    def enter(self, sibling=False):
        barrier = pltpu.get_barrier_semaphore()
        for dy, dx in ((0, 1), (0, -1), (1, 0), (-1, 0)):
            pl.semaphore_signal(barrier, inc=1, device_id=self.device(self.y + dy, self.x + dx), device_id_type=MESH)
        if sibling:
            pl.semaphore_signal(barrier, inc=1, device_id=self.sibling(), device_id_type=MESH)
        pl.semaphore_wait(barrier, 5 if sibling else 4)


def send(src, dst, sems, recvs, at, to):
    return pltpu.make_async_remote_copy(
        src_ref=src, dst_ref=dst, send_sem=sems.at[at], recv_sem=recvs.at[at], device_id=to, device_id_type=MESH
    )


def embed_kernel(side, gain_ref, look_ref, x_ref, n_ref, ring1, ring2, s1, r1, s2, r2):
    rows, dim = x_ref.shape
    plane = Plane(side, rows, dim // STREAMS)
    last = side - 1
    every = range(STREAMS)
    sent = []

    def go(c):
        c.start()
        sent.append(c)

    def scatter_first(k, s, j, src):
        return send(src, ring1.at[k, s, j], s1, r1, (k, s, j), plane.next_first(k))

    def scatter_second(k, m, src):
        return send(src, ring2.at[k, m], s2, r2, (k, m), plane.next_second(k))

    plane.enter()
    for j in range(side):
        for k in every:
            go(scatter_first(k, 0, j, plane.piece(look_ref, k, 1, 1 + j)))
    for s in range(last):
        for j in range(side):
            for k in every:
                held = ring1.at[k, s, j]
                scatter_first(k, s, j, held).wait_recv()
                held[...] += plane.piece(look_ref, k, 2 + s, 1 + j)[...]
            for k in every:
                held = ring1.at[k, s, j]
                if s < last - 1:
                    go(scatter_first(k, s + 1, j, held))
                elif j == 0:
                    go(scatter_second(k, 0, held))
    for j in range(1, side):
        for k in every:
            held = ring2.at[k, j - 1]
            scatter_second(k, j - 1, held).wait_recv()
            total = held[...] + ring1[k, last - 1, j]
            if j < last:
                held[...] = total
            else:
                x_ref[:, pl.ds(k * plane.cols, plane.cols)] = total
        if j < last:
            for k in every:
                go(scatter_second(k, j, ring2.at[k, j - 1]))

    strip = 16

    @pl.loop(0, rows // strip)
    def _(i):
        at = pl.ds(pl.multiple_of(i * strip, strip), strip)
        e = x_ref[at, :].astype(jnp.float32)
        r = lax.rsqrt(jnp.mean(e * e, axis=-1, keepdims=True) + EPS)
        n_ref[at, :] = (e * r * gain_ref[...].astype(jnp.float32)).astype(jnp.bfloat16)

    for c in sent:
        c.wait_send()


def gather_kernel(side, x_ref, d_ref, w_ref, out_ref, dh_ref, d_buf, t1, u1, t2, u2, own_sem, d_sem):
    rows, dim = x_ref.shape
    plane = Plane(side, rows, dim // STREAMS)
    last = side - 1
    every = range(STREAMS)

    def along_first(k, s, src):
        return send(src, plane.piece(out_ref, k, s, 0), t1, u1, (k, s), plane.next_first(k))

    def along_second(k, m, i, src):
        return send(src, plane.piece(out_ref, k, i, m), t2, u2, (k, m, i), plane.next_second(k))

    fetch = pltpu.make_async_copy(d_ref, d_buf, d_sem)
    fetch.start()
    plane.enter()
    for k in every:
        src = x_ref.at[:, pl.ds(k * plane.cols, plane.cols)]
        along_first(k, 0, src).start()
        along_second(k, 0, 0, src).start()
    keep = pltpu.make_async_copy(x_ref, out_ref.at[pl.ds(pl.multiple_of(plane.chip * rows, rows), rows), :], own_sem)
    keep.start()

    def arrived_second(k, m, i):
        p = plane.piece(out_ref, k, i, m + 1)
        along_second(k, m, i, p).wait_recv()

        @pl.when(m < last - 1)
        def _():
            along_second(k, m + 1, i, p).start()

    for s in range(last):
        for k in every:
            p = plane.piece(out_ref, k, s + 1, 0)
            along_first(k, s, p).wait_recv()
            if s < last - 1:
                along_first(k, s + 1, p).start()
            along_second(k, 0, s + 1, p).start()
        for k in every:
            arrived_second(k, 0, s)
    fetch.wait()
    steps = (last - 1) * side
    per = d_buf.shape[0] // steps

    @pl.loop(0, steps + 1)
    def _(i):
        t = i + last

        for k in every:
            arrived_second(k, t // side, lax.rem(t, side))

        @pl.when(i < steps)
        def _():
            at = pl.ds(pl.multiple_of(i * per, per), per)
            dh_ref[at, :] = lax.dot_general(
                d_buf[at, :], w_ref[...], (((1,), (1,)), ((), ())), preferred_element_type=jnp.float32
            ).astype(jnp.bfloat16)

    keep.wait()
    for k in every:
        for s in range(last):
            p = plane.piece(out_ref, k, s, 0)
            along_first(k, s, p).wait_send()
        for m in range(last):
            for i in range(side):
                p = plane.piece(out_ref, k, i, m)
                along_second(k, m, i, p).wait_send()


def embed(look, gain, rows, side):
    total, dim = look.shape
    cols, last = dim // STREAMS, side - 1
    dma = pltpu.SemaphoreType.DMA
    vmem = pl.BlockSpec(memory_space=pltpu.VMEM)
    line, block = dma((STREAMS, last)), dma((STREAMS, last, side))
    return pl.pallas_call(
        functools.partial(embed_kernel, side),
        out_shape=(jax.ShapeDtypeStruct((rows, dim), look.dtype), jax.ShapeDtypeStruct((rows, dim), look.dtype)),
        in_specs=[vmem, vmem],
        out_specs=(vmem, vmem),
        scratch_shapes=[
            pltpu.VMEM((STREAMS, last, side, rows, cols), look.dtype),
            pltpu.VMEM((STREAMS, last, rows, cols), look.dtype),
            block,
            block,
            line,
            line,
        ],
        compiler_params=pltpu.CompilerParams(collective_id=0, has_side_effects=True),
        cost_estimate=pl.CostEstimate(flops=100_000_000_000, bytes_accessed=4 * total * dim, transcendentals=0),
        name="embed",
    )(gain.reshape(1, dim), look)


def gather_and_multiply(x, d, w, side):
    rows, dim = x.shape
    total, width = d.shape[0], w.shape[0]
    last = side - 1
    dma = pltpu.SemaphoreType.DMA
    vmem = pl.BlockSpec(memory_space=pltpu.VMEM)
    line, block = dma((STREAMS, last)), dma((STREAMS, last, side))
    return pl.pallas_call(
        functools.partial(gather_kernel, side),
        out_shape=(jax.ShapeDtypeStruct((total, dim), x.dtype), jax.ShapeDtypeStruct((total, width), x.dtype)),
        in_specs=[vmem, pl.BlockSpec(memory_space=pl.ANY), vmem],
        out_specs=(pl.BlockSpec(memory_space=pl.ANY), vmem),
        scratch_shapes=[pltpu.VMEM((total, dim), d.dtype), line, line, block, block, dma(()), dma(())],
        compiler_params=pltpu.CompilerParams(collective_id=3, has_side_effects=True),
        cost_estimate=pl.CostEstimate(flops=100_000_000_000, bytes_accessed=4 * total * dim, transcendentals=0),
        name="gather_and_multiply",
    )(x, d, w)


def reduce_kernel(side, g_ref, v_ref, h_ref, w_ref, out_ref, y_ref, ring1, ring2, head, stage, s1, r1, s2, r2, ys):
    rows, dim = out_ref.shape
    plane = Plane(side, rows, dim // STREAMS)
    last = side - 1
    every = range(STREAMS)
    per = stage.shape[1]

    def scatter_first(k, s, j, src):
        return send(src, ring1.at[k, s, j], s1, r1, (k, s, j), plane.next_first(k))

    def scatter_second(k, m, src):
        return send(src, ring2.at[k, m], s2, r2, (k, m), plane.next_second(k))

    def term(k, a, b):
        cols = pl.ds(k * plane.cols, plane.cols)
        return lax.dot_general(
            g_ref[plane.block_rows(k, a, b), :], v_ref[cols, :], (((1,), (1,)), ((), ())), preferred_element_type=jnp.float32
        )

    def store(i, slot):
        rows_i = pl.ds(pl.multiple_of(i * per, per), per)
        return pltpu.make_async_copy(stage.at[slot], y_ref.at[rows_i, :], ys.at[slot])

    def take(k, s, j):
        held = ring1.at[k, s, j]
        scatter_first(k, s, j, held).wait_recv()
        held[...] += term(k, 2 + s, 1 + j)

    plane.enter()

    @pl.loop(0, side)
    def _(j):
        for k in every:
            head[k, j] = term(k, 1, 1 + j)
        for k in every:
            scatter_first(k, 0, j, head.at[k, j]).start()

    steps = (last - 1) * side

    @pl.loop(0, steps)
    def _(i):
        s, j, slot = i // side, lax.rem(i, side), lax.rem(i, 2)
        for k in every:
            take(k, s, j)
        for k in every:
            scatter_first(k, s + 1, j, ring1.at[k, s, j]).start()

        @pl.when(i >= 2)
        def _():
            store(i - 2, slot).wait()

        stage[slot] = jnp.dot(
            h_ref[pl.ds(pl.multiple_of(i * per, per), per), :], w_ref[...], preferred_element_type=jnp.float32
        )
        store(i, slot).start()

    @pl.loop(0, side)
    def _(j):
        for k in every:
            take(k, last - 1, j)

        @pl.when(j == 0)
        def _():
            for k in every:
                scatter_second(k, 0, ring1.at[k, last - 1, 0]).start()

    for j in range(1, side):
        for k in every:
            held = ring2.at[k, j - 1]
            scatter_second(k, j - 1, held).wait_recv()
            total = held[...] + ring1[k, last - 1, j]
            if j < last:
                held[...] = total
            else:
                out_ref[:, pl.ds(k * plane.cols, plane.cols)] = total
        if j < last:
            for k in every:
                scatter_second(k, j, ring2.at[k, j - 1]).start()

    @pl.loop(0, last * side)
    def _(i):
        for k in every:
            scatter_first(k, i // side, lax.rem(i, side), ring1.at[k, i // side, lax.rem(i, side)]).wait_send()

    for m in range(last):
        for k in every:
            scatter_second(k, m, ring2.at[k, m]).wait_send()
    for i in (steps - 2, steps - 1):
        store(i, i % 2).wait()


def reduce_and_multiply(g, v, h, w, rows, side):
    total, dim = g.shape[0], w.shape[1]
    f32 = jnp.float32
    cols, last = dim // STREAMS, side - 1
    per = total // ((last - 1) * side)
    dma = pltpu.SemaphoreType.DMA
    vmem = pl.BlockSpec(memory_space=pltpu.VMEM)
    anywhere = pl.BlockSpec(memory_space=pl.ANY)
    return pl.pallas_call(
        functools.partial(reduce_kernel, side),
        out_shape=(jax.ShapeDtypeStruct((rows, dim), f32), jax.ShapeDtypeStruct((total, dim), f32)),
        in_specs=[vmem] * 4,
        out_specs=(vmem, anywhere),
        scratch_shapes=[
            pltpu.VMEM((STREAMS, last, side, rows, cols), f32),
            pltpu.VMEM((STREAMS, last, rows, cols), f32),
            pltpu.VMEM((STREAMS, side, rows, cols), f32),
            pltpu.VMEM((2, per, dim), f32),
            dma((STREAMS, last, side)),
            dma((STREAMS, last, side)),
            dma((STREAMS, last)),
            dma((STREAMS, last)),
            dma((2,)),
        ],
        compiler_params=pltpu.CompilerParams(collective_id=1, has_side_effects=True),
        cost_estimate=pl.CostEstimate(flops=100_000_000_000, bytes_accessed=12 * total * dim, transcendentals=0),
        name="reduce_and_multiply",
    )(g, v, h, w)


def spread_kernel(side, dx_ref, out_ref, t1, u1, t2, u2, v1, w1, v2, w2, v0, w0, own_sem):
    rows, dim = dx_ref.shape
    plane = Plane(side, rows, dim // STREAMS, cores=2)
    last = side - 1
    every = range(STREAMS)
    sent = []

    def go(c):
        c.start()
        sent.append(c)

    def here(k, a, b):
        return plane.piece(out_ref, k, a, b, plane.core)

    def along_first(k, s, src):
        return send(src, here(k, s, 0), t1, u1, (k, s), plane.next_first(k))

    def along_second(k, m, i, src):
        return send(src, here(k, i, m), t2, u2, (k, m, i), plane.next_second(k))

    def across(k, a, b, core, sems, recvs, at):
        p = plane.piece(out_ref, k, a, b, core)
        return send(p, p, sems, recvs, at, plane.sibling())

    plane.enter(sibling=True)
    mine = out_ref.at[pl.ds(pl.multiple_of(plane.rank * rows, rows), rows), :]
    keep = pltpu.make_async_copy(dx_ref, mine, own_sem)
    keep.start()
    for k in every:
        src = dx_ref.at[:, pl.ds(k * plane.cols, plane.cols)]
        go(along_first(k, 0, src))
        go(along_second(k, 0, 0, src))
    go(send(dx_ref, mine, v0, w0, 0, plane.sibling()))

    def arrived_second(k, m, i):
        p = here(k, i, m + 1)
        along_second(k, m, i, p).wait_recv()
        if m < last - 1:
            go(along_second(k, m + 1, i, p))
        go(across(k, i, m + 1, plane.core, v2, w2, (k, m, i)))

    for s in range(last):
        for k in every:
            p = here(k, s + 1, 0)
            along_first(k, s, p).wait_recv()
            if s < last - 1:
                go(along_first(k, s + 1, p))
            go(along_second(k, 0, s + 1, p))
            go(across(k, s + 1, 0, plane.core, v1, w1, (k, s)))
        for k in every:
            arrived_second(k, 0, s)
    for m in range(last):
        for i in range(last if m == 0 else 0, side):
            for k in every:
                arrived_second(k, m, i)

    other = 1 - plane.core
    theirs = out_ref.at[pl.ds(pl.multiple_of((plane.chip * 2 + other) * rows, rows), rows), :]
    send(dx_ref, theirs, v0, w0, 0, plane.sibling()).wait_recv()
    for k in every:
        for s in range(last):
            across(k, s + 1, 0, other, v1, w1, (k, s)).wait_recv()
        for m in range(last):
            for i in range(side):
                across(k, i, m + 1, other, v2, w2, (k, m, i)).wait_recv()
    keep.wait()
    for c in sent:
        c.wait_send()


def spread(dx, n_dev, side):
    rows, dim = dx.shape
    last = side - 1
    dma = pltpu.SemaphoreType.DMA
    line, block = dma((STREAMS, last)), dma((STREAMS, last, side))
    return pl.pallas_call(
        functools.partial(spread_kernel, side),
        out_shape=jax.ShapeDtypeStruct((n_dev * rows, dim), dx.dtype),
        in_specs=[pl.BlockSpec(memory_space=pltpu.VMEM)],
        out_specs=pl.BlockSpec(memory_space=pl.ANY),
        scratch_shapes=[line, line, block, block, line, line, block, block, dma((1,)), dma((1,)), dma(())],
        compiler_params=pltpu.CompilerParams(collective_id=2, has_side_effects=True),
        cost_estimate=pl.CostEstimate(flops=100_000_000_000, bytes_accessed=4 * n_dev * rows * dim, transcendentals=0),
        name="spread",
    )(dx)


def solution(mesh):
    n_dev = mesh.shape["tp"]
    planes = [list(range(c, n_dev, 2)) for c in range(2)]
    side = math.isqrt(n_dev // 2)
    swap = [(i, i ^ 1) for i in range(n_dev)]
    f32, bf16 = jnp.float32, jnp.bfloat16

    def gather_plane(v):
        return lax.all_gather(v, "tp", axis=0, tiled=True, axis_index_groups=planes)

    def scatter_plane(v):
        return lax.psum_scatter(v, "tp", scatter_dimension=0, tiled=True, axis_index_groups=planes)

    def dot(a, b, ca, cb):
        return lax.dot_general(a, b, (((ca,), (cb,)), ((), ())), preferred_element_type=f32)

    def shard_step(token_ids, emb_table, norm_gain, w_in, w_out, d_out):
        rank = lax.axis_index("tp")
        core = rank % 2
        rows = d_out.shape[0]
        width = w_in.shape[1]
        vocab = emb_table.shape[0]
        own_base = rank * vocab
        sib_base = (rank + 1 - 2 * core) * vocab
        ids_blocks = token_ids.reshape(n_dev // 2, 2, rows)
        ids_plane = lax.dynamic_index_in_dim(ids_blocks, core, axis=1, keepdims=False).reshape(-1, 1)
        vocab_col = lax.broadcasted_iota(jnp.int32, (1, vocab), 1)
        vocab_row = lax.broadcasted_iota(jnp.int32, (vocab, 1), 0)
        gain_f32 = norm_gain.astype(f32)

        table_sib = lax.ppermute(emb_table, "tp", swap)
        w_out2 = jnp.concatenate([w_out, lax.ppermute(w_out, "tp", swap)], axis=0)
        w_in2 = jnp.concatenate([w_in, lax.ppermute(w_in, "tp", swap)], axis=1)

        d_full = gather_plane(d_out)

        own = (ids_plane - own_base == vocab_col).astype(bf16)
        sib = (ids_plane - sib_base == vocab_col).astype(bf16)
        look = (dot(own, emb_table, 1, 0) + dot(sib, table_sib, 1, 0)).astype(bf16)
        emb, normed_local = embed(look, norm_gain, rows, side)
        normed, d_hidden = gather_and_multiply(normed_local, d_full, w_out2, side)
        emb = emb.astype(f32)
        inv = lax.rsqrt(jnp.mean(emb * emb, axis=-1, keepdims=True) + EPS)

        pre_act = dot(normed, w_in2, 1, 0).astype(bf16)
        act_f32, gelu_vjp = jax.vjp(jax.nn.gelu, pre_act.astype(f32))
        hidden = act_f32.astype(bf16)
        (d_pre_f32,) = gelu_vjp(d_hidden.astype(f32))
        d_pre = d_pre_f32.astype(bf16)
        d_normed, y_part = reduce_and_multiply(d_pre, w_in2, hidden, w_out2, rows, side)
        y_sum = scatter_plane(y_part)

        d_scaled = d_normed * gain_f32
        row_proj = jnp.mean(d_scaled * emb, axis=-1, keepdims=True)
        d_emb = (d_out.astype(f32) + inv * (d_scaled - emb * inv * inv * row_proj)).astype(bf16)
        d_emb_full = spread(d_emb, n_dev, side)

        late = lax.optimization_barrier((emb, normed, d_pre, hidden, d_full, d_emb_full))
        emb, normed, d_pre, hidden, d_full, d_emb_full = late
        d_w_in2 = dot(normed, d_pre, 0, 0)
        d_w_out2 = dot(hidden, d_full, 0, 0)
        d_w_in = d_w_in2[:, :width] + lax.ppermute(d_w_in2[:, width:], "tp", swap)
        d_w_out = d_w_out2[:width] + lax.ppermute(d_w_out2[width:], "tp", swap)

        block_out = (emb + y_sum).astype(bf16)
        hit = (token_ids.reshape(1, -1) - own_base == vocab_row).astype(bf16)
        d_table = dot(hit, d_emb_full, 1, 0)
        return block_out, d_table, d_w_in, d_w_out

    return jax.shard_map(
        shard_step,
        mesh=mesh,
        in_specs=(P("dp"), P("tp", None), P(None), P(None, "tp"), P("tp", None), P(("dp", "tp"), None)),
        out_specs=(P(("dp", "tp"), None), P(("dp", "tp"), None), P("dp", "tp"), P(("dp", "tp"), None)),
        check_vma=False,
    )
```
